32 devices in a mesh: grp: 2 (over y), band: 4 (over z), mem: 2 (over x), fld: 2 (over core).
Axes of the slice: x: 2, y: 2, z: 4, core: 2. Of those that a mesh axis runs over, the one named last changes fastest.
Arguments:
- surface_fields: bfloat16 [16, 8, 8, 65536], P(('grp', 'mem'), 'fld', None, 'band'), parts along dimension 0, may hold values from -8 to 8
- land_mask: int32 [65536], P('band'), may hold values from 0 to 1, as said below
- source_area: float32 [65536], P('band'), may hold values from 0.5 to 1.5
- target_area: float32 [16384], P('band'), may hold values from 0.75 to 1.25
- weight_tiles: bfloat16 [16, 128, 128], replicated, may hold values from -1 to 1
- tile_of: int32 [128, 24], P('band'), may hold values from 0 to 15
- block_of: int32 [128, 24], P('band'), may hold values from 0 to 191, as said below
- live_slots: int32 [128], P('band'), may hold values from 1 to 24, as said below
Outputs:
- regridded: float32 [16, 8, 8, 16384], P(('grp', 'mem'), 'fld', None, 'band'), parts along dimension 0
- conserved: float32 [16, 8, 8], P(('grp', 'mem'), 'fld'), parts along dimension 0
- ensemble: float32 [16, 8], P(('grp', 'fld')), parts along dimension 0
The draws below stay inside these ranges and needn't reach their ends.
There are 2 independent parts, one for each index of `grp`. The reference program is written for one: setup_inputs(seed, part) draws one part's arguments, and reference() takes and returns one part's arrays. A program takes and returns all parts, laid end to end along the dimension named above; an argument that names none is the same for every part. Nothing has to cross between parts.
Inputs may be any that keep to these rules, and one draw needn't show every extreme that they name: `land_mask`: 1 marks ocean, 0 land. `block_of`: for the target block at place j (0 to 31) within its band, every entry lies in 4 * j to 4 * j + 4 + 2 * 32 - 1; values under 32 name the lower band's last blocks, values from 160 on the higher band's first blocks. `live_slots`: slots from this count on are unused.
All inputs are finite; a program needn't handle non-finite values.
Results may differ from the reference program's by a relative error of at most 0.0014.
Values may be sent and summed in bfloat16 or wider, within the bound.
A program may use at most 64 MiB of HBM per device.

```python
import jax
import jax.numpy as jnp
from jax import lax

MEMBERS = 8
FIELDS = 8
SNAPSHOTS = 8
TILE_CELLS = 128
TGT_BLK_DEV = 32
STRIDE = 4
HALO_BLK = 32
SLOT_COUNT = 24
TILE_COUNT = 16
SRC_BLK_DEV = 128
SRC_BLOCKS = 512
TGT_BLOCKS = 128
SRC_CELLS = 65536
TGT_CELLS = 16384


def draw_surface_fields(key, part):
    first_key, second_key, third_key = jax.random.split(key, 3)
    shape = (MEMBERS, FIELDS, SNAPSHOTS, SRC_BLOCKS, TILE_CELLS)
    offset = jax.random.uniform(first_key, (MEMBERS, FIELDS, SNAPSHOTS, 1, 1), jnp.float32, -1.0, 1.0)
    noise = jnp.clip(jax.random.normal(third_key, shape, jnp.float32), -5.0, 5.0)
    regional = 0.5 * jnp.clip(jax.random.normal(second_key, (MEMBERS, FIELDS, SNAPSHOTS, SRC_BLOCKS, 1), jnp.float32), -2.0, 2.0)
    values = offset + regional + noise
    return values.reshape(MEMBERS, FIELDS, SNAPSHOTS, SRC_CELLS).astype(jnp.bfloat16)


def draw_land_mask(key, part):
    first_key, second_key, third_key = jax.random.split(key, 3)
    band_count = SRC_CELLS // (SRC_BLK_DEV * TILE_CELLS)
    band_level = jax.random.randint(first_key, (band_count, 1, 1), 25, 101)
    region_level = jax.random.randint(second_key, (band_count, SRC_BLK_DEV, 1), 40, 101)
    cell_draw = jax.random.randint(third_key, (band_count, SRC_BLK_DEV, TILE_CELLS), 0, 10000)
    ocean = (cell_draw < band_level * region_level).astype(jnp.int32)
    return ocean.reshape(SRC_CELLS)


def draw_weight_tiles(key, part):
    fan = SLOT_COUNT * TILE_CELLS
    shape = (TILE_COUNT, TILE_CELLS, TILE_CELLS)
    noise = jnp.clip(jax.random.normal(key, shape, jnp.float32), -5.0, 5.0)
    mean_part = 1.0
    return ((mean_part + noise * jnp.sqrt(jnp.float32(fan))) / fan).astype(jnp.bfloat16)


def draw_block_of(key, part):
    position = jnp.arange(TGT_BLOCKS, dtype=jnp.int32) % TGT_BLK_DEV
    offsets = jax.random.randint(key, (TGT_BLOCKS, SLOT_COUNT), 0, STRIDE + 2 * HALO_BLK)
    picks = STRIDE * position[:, None] + offsets
    picks = picks.at[0, 0].set(0)
    picks = picks.at[TGT_BLOCKS - 1, 0].set(STRIDE * TGT_BLK_DEV + 2 * HALO_BLK - 1)
    return picks.astype(jnp.int32)


def draw_live_slots(key, part):
    first_key, second_key = jax.random.split(key, 2)
    band_count = TGT_BLOCKS // TGT_BLK_DEV
    tops = jax.random.randint(first_key, (band_count,), SLOT_COUNT // 4 + 1, SLOT_COUNT + 1)
    band_top = jnp.repeat(tops, TGT_BLK_DEV)
    counts = jax.random.randint(second_key, (TGT_BLOCKS,), 1, band_top + 1)
    return counts.at[0].set(SLOT_COUNT).astype(jnp.int32)


def set_ends(array, stream_key, least, largest):
    longest = array.shape.index(max(array.shape))
    spots = []
    for shift in (0, 1):
        where = [jax.random.randint(jax.random.fold_in(stream_key, axis), (), 0, length) for axis, length in enumerate(array.shape)]
        where[longest] = (where[longest] + shift) % array.shape[longest]
        spots.append(tuple(where))
    return array.at[spots[0]].set(least).at[spots[1]].set(largest)


def level_of(key, extent, pieces, least, high):
    factor_of, own = 1.0, jax.random.fold_in(key, 6)
    for dim, blocks in pieces:
        draws = jnp.exp(jax.random.uniform(jax.random.fold_in(own, dim), (blocks,), jnp.float32, least / len(pieces), high / len(pieces)))
        factor_of = factor_of * jnp.repeat(draws, extent[dim] // blocks).reshape([-1 if axis == dim else 1 for axis in range(len(extent))])
    return factor_of


def setup_inputs(seed: int = 0, part: int = 0) -> dict:
    splits = jax.random.split(jax.random.key(seed), 9)
    own_keys = jax.random.split(jax.random.fold_in(splits[8], part), 9)
    return {
        "surface_fields": draw_surface_fields(jax.random.fold_in(jax.random.fold_in(splits[8], part), 71), part),
        "land_mask": draw_land_mask(jax.random.fold_in(splits[8], 71), part),
        "source_area": jnp.clip(0.5 + 1.0 * jax.random.uniform(splits[2], (SRC_CELLS,), jnp.float32) ** level_of(splits[2], (SRC_CELLS,), ((0, 4),), -0.2, 0.2), 0.5, 1.5),
        "target_area": jnp.clip(0.75 + 0.5 * jax.random.uniform(splits[3], (TGT_CELLS,), jnp.float32) ** level_of(splits[3], (TGT_CELLS,), ((0, 4),), -0.2, 0.2), 0.75, 1.25),
        "weight_tiles": draw_weight_tiles(jax.random.fold_in(splits[8], 71), part),
        "tile_of": set_ends(jax.random.randint(splits[5], (TGT_BLOCKS, SLOT_COUNT), 0, TILE_COUNT), jax.random.fold_in(splits[5], 1), 0, TILE_COUNT - 1).astype(jnp.int32),
        "block_of": draw_block_of(jax.random.fold_in(splits[8], 71), part),
        "live_slots": draw_live_slots(jax.random.fold_in(splits[8], 71), part),
    }


def reference(surface_fields, land_mask, source_area, target_area, weight_tiles, tile_of, block_of, live_slots):
    columns = MEMBERS * FIELDS * SNAPSHOTS
    weighted = (source_area * land_mask.astype(jnp.float32) * surface_fields.astype(jnp.float32)).astype(jnp.bfloat16)
    flat = weighted.reshape(columns, SRC_BLOCKS, TILE_CELLS)
    padding = jnp.zeros((columns, HALO_BLK, TILE_CELLS), jnp.bfloat16)
    padded = jnp.concatenate([padding, flat, padding], axis=1)
    owner = jnp.arange(TGT_BLOCKS, dtype=jnp.int32) // TGT_BLK_DEV
    picks = (owner[:, None] * SRC_BLK_DEV + block_of).astype(jnp.int32)

    def one_slot(running, position):
        chosen = jnp.take(padded, picks[:, position], axis=1).astype(jnp.float32)
        weights = jnp.take(weight_tiles, tile_of[:, position], axis=0).astype(jnp.float32)
        usable = (position < live_slots)[:, None, None]
        weights = jnp.where(usable, weights, jnp.zeros((), jnp.float32))
        running = running + jnp.einsum("cnb,nbd->cnd", chosen, weights, precision=lax.Precision.HIGHEST)
        return running, None

    start = jnp.zeros((columns, TGT_BLOCKS, TILE_CELLS), jnp.float32)
    raw_sums, unused = lax.scan(one_slot, start, jnp.arange(SLOT_COUNT, dtype=jnp.int32))
    raw_sums = raw_sums.reshape(columns, TGT_CELLS)
    source_total = jnp.sum(weighted.reshape(columns, SRC_CELLS).astype(jnp.float32), axis=1)
    target_total = jnp.sum(raw_sums, axis=1)
    area_total = jnp.sum(target_area)
    regridded = raw_sums / target_area[None, :] + ((source_total - target_total) / area_total)[:, None]
    conserved = (source_total / area_total).reshape(MEMBERS, FIELDS, SNAPSHOTS)
    ensemble = jnp.sum(conserved, axis=0) / MEMBERS
    return regridded.reshape(MEMBERS, FIELDS, SNAPSHOTS, TGT_CELLS), conserved, ensemble
```

```python
import functools

import jax
import jax.numpy as jnp
from jax import lax
from jax.experimental import pallas as pl
from jax.experimental.pallas import tpu as pltpu
from jax.sharding import PartitionSpec as P

HALO_BLK = 32
GROUP = 8
SEND_TYPE = jnp.float32
MESH = pl.DeviceIdType.MESH
VMEM = pl.BlockSpec(memory_space=pltpu.VMEM)
SMEM = pl.BlockSpec(memory_space=pltpu.SMEM)


def row_of(sums):
    return jnp.sum(sums.T, axis=0, keepdims=True)


def weigh_kernel(tile, fields_ref, mask_ref, area_ref, out_ref, total_ref):
    scale = area_ref[...] * mask_ref[...].astype(jnp.float32)
    columns = total_ref.shape[0]

    @pl.when(pl.program_id(0) == 0)
    def _():
        total_ref[...] = jnp.zeros_like(total_ref)

    running = total_ref[...]
    for n in range(out_ref.shape[0]):
        part = fields_ref[:, :, n * tile:(n + 1) * tile].astype(jnp.float32)
        part = part.reshape(columns, tile) * scale[:, n * tile:(n + 1) * tile]
        part = part.astype(jnp.bfloat16)
        out_ref[n] = part
        running = running + part.astype(jnp.float32)
    total_ref[...] = running


def weigh(fields, mask, area, tile, steps):
    rows, snaps, cells = fields.shape
    columns, blocks = rows * snaps, cells // tile
    chunk = cells // steps
    return pl.pallas_call(
        functools.partial(weigh_kernel, tile),
        grid=(steps,),
        in_specs=[
            pl.BlockSpec((rows, snaps, chunk), lambda i: (0, 0, i)),
            pl.BlockSpec((1, chunk), lambda i: (0, i)),
            pl.BlockSpec((1, chunk), lambda i: (0, i)),
        ],
        out_specs=(
            pl.BlockSpec((blocks // steps, columns, tile), lambda i: (i, 0, 0)),
            pl.BlockSpec((columns, tile), lambda i: (0, 0)),
        ),
        out_shape=(
            jax.ShapeDtypeStruct((blocks, columns, tile), jnp.bfloat16),
            jax.ShapeDtypeStruct((columns, tile), jnp.float32),
        ),
        cost_estimate=pl.CostEstimate(
            flops=4 * columns * cells, bytes_accessed=4 * columns * cells, transcendentals=0
        ),
    )(fields, mask, area)


def list_pairs(first, count, slots, table, shift, low, high, zero_tile, lists, start):
    tiles, blocks, live = table
    list_b, list_w, list_t = lists

    def one_target(n, place):
        used = live(n)
        for i in range(slots // 2 + 1):
            list_t[place // 2 + i] = first + n
        for k in range(slots):
            block = blocks(n, k) - shift
            keep = (k < used) & (block >= low) & (block < high)
            list_b[place] = block
            list_w[place] = tiles(n, k)
            place = place + keep.astype(jnp.int32)
        list_b[place] = low
        list_w[place] = zero_tile
        return place + lax.rem(place, 2)

    return lax.fori_loop(0, count, one_target, start)


def run_pairs(source, tiles, lists, entries, zero_tile, low, acc):
    list_b, list_w, list_t = lists
    for i in range(2 * GROUP):
        list_b[entries + i] = low
        list_w[entries + i] = zero_tile
    for i in range(GROUP):
        list_t[entries // 2 + i] = 0

    def one_group(g, carry):
        for u in range(GROUP):
            p = g * GROUP + u
            left = jnp.concatenate(
                [source[list_b[2 * p]], source[list_b[2 * p + 1]]], axis=1
            )
            right = jnp.concatenate(
                [tiles[list_w[2 * p]], tiles[list_w[2 * p + 1]]], axis=0
            )
            t = list_t[p]
            acc[t] = acc[t] + jnp.dot(left, right, preferred_element_type=jnp.float32)
        return carry

    lax.fori_loop(0, (entries // 2 + GROUP - 1) // GROUP, one_group, 0)


def fill_tiles(tiles_ref, held):
    count = tiles_ref.shape[0]
    held[0:count] = tiles_ref[...]
    held[count] = jnp.zeros(held.shape[1:], held.dtype)


def edge_kernel(
    edge, slots, own, upper_ref, lower_ref, source, tiles_ref, up_ref, down_ref, sum_ref,
    held, acc, list_b, list_w, list_t,
):
    fill_tiles(tiles_ref, held)
    zero_tile = tiles_ref.shape[0]
    acc[...] = jnp.zeros_like(acc)
    lists = (list_b, list_w, list_t)

    def table(ref):
        return (
            lambda n, k: ref[n, k],
            lambda n, k: ref[n, slots + k],
            lambda n: ref[n, 2 * slots],
        )

    place = list_pairs(
        0, edge, slots, table(upper_ref), HALO_BLK - own, own - HALO_BLK, own, zero_tile, lists, 0
    )
    place = list_pairs(
        edge, edge, slots, table(lower_ref), own + HALO_BLK, 0, HALO_BLK, zero_tile, lists, place
    )
    run_pairs(source, held, lists, place, zero_tile, 0, acc)
    up_ref[...] = acc[0:edge].astype(up_ref.dtype)
    down_ref[...] = acc[edge:2 * edge].astype(down_ref.dtype)
    sum_ref[...] = jnp.sum(acc[...], axis=0)


def list_scratch(targets, slots):
    size = targets * (slots + 2) + 4 * GROUP + slots
    return [
        pltpu.SMEM((size,), jnp.int32),
        pltpu.SMEM((size,), jnp.int32),
        pltpu.SMEM((size,), jnp.int32),
    ]


def edges(upper, lower, source, tiles, edge, slots):
    own, columns, tile = source.shape
    part = jax.ShapeDtypeStruct((edge, columns, tile), SEND_TYPE)
    return pl.pallas_call(
        functools.partial(edge_kernel, edge, slots, own),
        in_specs=[SMEM, SMEM, VMEM, VMEM],
        out_specs=(VMEM, VMEM, VMEM),
        out_shape=(part, part, jax.ShapeDtypeStruct((columns, tile), jnp.float32)),
        scratch_shapes=[
            pltpu.VMEM((tiles.shape[0] + 1, tile, tile), tiles.dtype),
            pltpu.VMEM((2 * edge, columns, tile), jnp.float32),
        ] + list_scratch(2 * edge, slots),
        cost_estimate=pl.CostEstimate(
            flops=2 * 4 * edge * columns * tile * tile, bytes_accessed=4 << 20, transcendentals=0
        ),
    )(upper, lower, source, tiles)


def own_kernel(
    tile_of, block_of, live_ref, source, tiles_ref, src_ref, edge_ref, area_ref, raw_ref, row_ref,
    held, list_b, list_w, list_t,
):
    targets, slots = tile_of.shape
    own = source.shape[0]
    zero_tile = tiles_ref.shape[0]
    fill_tiles(tiles_ref, held)
    raw_ref[...] = jnp.zeros_like(raw_ref)
    lists = (list_b, list_w, list_t)
    table = (
        lambda n, k: tile_of[n, k],
        lambda n, k: block_of[n, k],
        lambda n: live_ref[n],
    )
    place = list_pairs(0, targets, slots, table, HALO_BLK, 0, own, zero_tile, lists, 0)
    run_pairs(source, held, lists, place, zero_tile, 0, raw_ref)
    columns = src_ref.shape[0]
    row_ref[0:1, :] = row_of(src_ref[...])
    row_ref[1:2, :] = row_of(jnp.sum(raw_ref[...], axis=0) + edge_ref[...])
    row_ref[2:3, :] = jnp.broadcast_to(jnp.sum(area_ref[...], axis=1, keepdims=True), (1, columns))
    row_ref[3:8, :] = jnp.zeros((5, columns), jnp.float32)


def own_targets(tile_of, block_of, live, source, tiles, src_sum, edge_sum, area):
    own, columns, tile = source.shape
    targets, slots = tile_of.shape
    return pl.pallas_call(
        own_kernel,
        in_specs=[SMEM, SMEM, SMEM, VMEM, VMEM, VMEM, VMEM, VMEM],
        out_specs=(VMEM, VMEM),
        out_shape=(
            jax.ShapeDtypeStruct((targets, columns, tile), jnp.float32),
            jax.ShapeDtypeStruct((8, columns), jnp.float32),
        ),
        scratch_shapes=[pltpu.VMEM((tiles.shape[0] + 1, tile, tile), tiles.dtype)]
        + list_scratch(targets, slots),
        cost_estimate=pl.CostEstimate(
            flops=2 * targets * slots * columns * tile * tile,
            bytes_accessed=6 << 20,
            transcendentals=0,
        ),
    )(tile_of, block_of, live, source, tiles, src_sum, edge_sum, area)


def totals_kernel(bands, mems, row_ref, out_ref, fix_ref, landed, send_sem, recv_sem):
    band, mem = lax.axis_index("band"), lax.axis_index("mem")
    count = bands * mems
    me = mem * bands + band

    def place(step):
        other = lax.rem(me + step, count)
        return other, {"mem": other // bands, "band": lax.rem(other, bands)}

    barrier = pltpu.get_barrier_semaphore()

    def greet(step, carry):
        pl.semaphore_signal(barrier, inc=1, device_id=place(step)[1], device_id_type=MESH)
        return carry

    lax.fori_loop(1, count, greet, 0)
    pl.semaphore_wait(barrier, count - 1)

    def copy(step):
        return pltpu.make_async_remote_copy(
            src_ref=row_ref,
            dst_ref=landed.at[step],
            send_sem=send_sem.at[step],
            recv_sem=recv_sem.at[step],
            device_id=place(step)[1],
            device_id_type=MESH,
        )

    def begin(step, carry):
        copy(step).start()
        return carry

    def finish(step, carry):
        copy(step).wait()
        return carry

    lax.fori_loop(1, count, begin, 0)
    landed[0] = row_ref[...]
    lax.fori_loop(1, count, finish, 0)
    for m in range(mems):
        total = jnp.zeros(row_ref.shape, jnp.float32)
        for b in range(bands):
            sender = m * bands + b
            total = total + landed[lax.rem(me - sender + count, count)]
        out_ref[m] = total
    mine = out_ref[mem]
    fix = (mine[0:1, :] - mine[1:2, :]) / mine[2:3, :]
    fix_ref[...] = jnp.broadcast_to(fix, (fix_ref.shape[1], fix.shape[1])).T


def exchange_totals(rows, tile):
    bands, mems = lax.axis_size("band"), lax.axis_size("mem")
    columns = rows.shape[1]
    return pl.pallas_call(
        functools.partial(totals_kernel, bands, mems),
        in_specs=[VMEM],
        out_specs=(VMEM, VMEM),
        out_shape=(
            jax.ShapeDtypeStruct((mems, 8, columns), jnp.float32),
            jax.ShapeDtypeStruct((columns, tile), jnp.float32),
        ),
        scratch_shapes=[
            pltpu.VMEM((bands * mems, 8, columns), jnp.float32),
            pltpu.SemaphoreType.DMA((bands * mems,)),
            pltpu.SemaphoreType.DMA((bands * mems,)),
        ],
        compiler_params=pltpu.CompilerParams(collective_id=0, has_side_effects=True),
    )(rows)


def finish_kernel(raw_ref, low_ref, high_ref, area_ref, fix_ref, out_ref):
    step, last = pl.program_id(0), pl.num_programs(0) - 1
    count, columns, tile = raw_ref.shape
    use_low = step == 0
    use_high = step == last
    for n in range(count):
        value = raw_ref[n]
        value = value + jnp.where(use_low, low_ref[n].astype(jnp.float32), 0.0)
        value = value + jnp.where(use_high, high_ref[n].astype(jnp.float32), 0.0)
        value = value / area_ref[:, n * tile:(n + 1) * tile] + fix_ref[...]
        out_ref[:, :, n * tile:(n + 1) * tile] = value.reshape(out_ref.shape[0], out_ref.shape[1], tile)


def finish(raw, low, high, area, fix, rows, snaps):
    targets, columns, tile = raw.shape
    edge = low.shape[0]
    return pl.pallas_call(
        finish_kernel,
        grid=(targets // edge,),
        in_specs=[
            pl.BlockSpec((edge, columns, tile), lambda i: (i, 0, 0)),
            pl.BlockSpec((edge, columns, tile), lambda i: (0, 0, 0)),
            pl.BlockSpec((edge, columns, tile), lambda i: (0, 0, 0)),
            pl.BlockSpec((1, edge * tile), lambda i: (0, i)),
            pl.BlockSpec((columns, tile), lambda i: (0, 0)),
        ],
        out_specs=pl.BlockSpec((rows, snaps, edge * tile), lambda i: (0, 0, i)),
        out_shape=jax.ShapeDtypeStruct((rows, snaps, targets * tile), jnp.float32),
    )(raw, low, high, area, fix)


def on_device(
    surface_fields, land_mask, source_area, target_area, weight_tiles, tile_of, block_of, live_slots
):
    members, fields, snaps, cells = surface_fields.shape
    tile = weight_tiles.shape[1]
    targets, slots = tile_of.shape
    own = cells // tile
    edge = HALO_BLK // (own // targets)
    bands = lax.axis_size("band")
    up = [(i, i + 1) for i in range(bands - 1)]
    down = [(j, i) for i, j in up]

    table = jnp.concatenate([tile_of, block_of, live_slots[:, None]], axis=1)
    upper = lax.ppermute(table[:edge], "band", down)
    lower = lax.ppermute(table[targets - edge:], "band", up)

    area = target_area.reshape(1, targets * tile)
    source, src_sum = weigh(
        surface_fields.reshape(members * fields, snaps, cells),
        land_mask.reshape(1, cells),
        source_area.reshape(1, cells),
        tile,
        8,
    )
    to_upper, to_lower, edge_sum = edges(upper, lower, source, weight_tiles, edge, slots)
    low = lax.ppermute(to_upper, "band", up)
    high = lax.ppermute(to_lower, "band", down)
    raw, rows = own_targets(
        tile_of, block_of, live_slots, source, weight_tiles, src_sum, edge_sum, area
    )
    totals, fix = exchange_totals(rows, tile)
    regridded = finish(raw, low, high, area, fix, members * fields, snaps)
    means = totals[:, 0] / totals[:, 2]
    conserved = lax.dynamic_index_in_dim(means, lax.axis_index("mem"), 0, keepdims=False)
    mems = means.shape[0]
    ensemble = jnp.sum(means.reshape(mems * members, fields, snaps), axis=0) / (mems * members)
    return (
        regridded.reshape(members, fields, snaps, targets * tile),
        conserved.reshape(members, fields, snaps),
        ensemble,
    )


def solution(mesh):
    placed = (
        P(("grp", "mem"), "fld", None, "band"),
        P("band"),
        P("band"),
        P("band"),
        P(),
        P("band", None),
        P("band", None),
        P("band"),
    )
    return jax.shard_map(
        on_device,
        mesh=mesh,
        in_specs=placed,
        out_specs=(
            P(("grp", "mem"), "fld", None, "band"),
            P(("grp", "mem"), "fld", None),
            P(("grp", "fld"), None),
        ),
        check_vma=False,
    )
```

```python
import functools

import jax
import jax.numpy as jnp
from jax import lax
from jax.experimental import pallas as pl
from jax.experimental.pallas import tpu as pltpu
from jax.sharding import PartitionSpec as P

HALO_BLK = 32
OWN_UNROLL = 2
SEND_TYPE = jnp.float32
MESH = pl.DeviceIdType.MESH
HBM = pl.BlockSpec(memory_space=pltpu.HBM)
VMEM = pl.BlockSpec(memory_space=pltpu.VMEM)


def row_of(sums):
    return jnp.sum(sums.T, axis=0, keepdims=True)


def slot_dot(source, held, table, n, slots, shift, low, high):
    tiles, blocks, live = table
    used, zero_tile = live(n), held.shape[0] - 1
    left, right = [], []
    for k in range(slots):
        block = blocks(k, n) - shift
        keep = (k < used) & (block >= low) & (block < high)
        left.append(source[jnp.where(keep, block, low)])
        right.append(held[jnp.where(keep, tiles(k, n), zero_tile)])
    return jnp.dot(
        jnp.concatenate(left, axis=1),
        jnp.concatenate(right, axis=0),
        preferred_element_type=jnp.float32,
    )


def main_kernel(
    bands, mems, edge,
    fields, mask_h, area_h, target_area_h, tiles, tile_h, block_h, live_h,
    raw, totals, fix_ref,
    mask, area, target_area, tile_s, block_s, live_s,
    stage, source, held, made, came, rows, landed, target_sum,
    tile_in, block_in, live_in, tile_n, block_n, live_n,
    load_sem, small_sem, list_sem, table_send, table_recv, edge_send, edge_recv, row_send, row_recv,
):
    band, mem = lax.axis_index("band"), lax.axis_index("mem")
    count = bands * mems
    me = mem * bands + band
    own, columns, tile = source.shape
    slots, targets = tile_h.shape
    has_low, has_high = band > 0, band < bands - 1
    chunk = HALO_BLK * tile
    chunks = own // HALO_BLK
    order = [0, chunks - 1] + list(range(1, chunks - 1))

    loads = [
        pltpu.make_async_copy(
            fields.at[:, :, pl.ds(c * chunk, chunk)],
            stage.at[:, :, pl.ds(c * chunk, chunk)],
            load_sem.at[c],
        )
        for c in range(chunks)
    ]
    small = [
        pltpu.make_async_copy(a, b, small_sem.at[i])
        for i, (a, b) in enumerate((
            (mask_h, mask),
            (area_h, area),
            (tiles, held.at[pl.ds(0, tiles.shape[0])]),
            (tile_h, tile_s),
            (block_h, block_s),
            (live_h, live_s),
            (target_area_h, target_area),
        ))
    ]
    small[0].start()
    small[1].start()
    for c in order[:2]:
        loads[c].start()
    for copy in small[2:]:
        copy.start()
    for c in order[2:]:
        loads[c].start()

    def place(step):
        other = lax.rem(me + step, count)
        return {"mem": other // bands, "band": lax.rem(other, bands)}

    barrier = pltpu.get_barrier_semaphore()

    def greet(step, carry):
        pl.semaphore_signal(barrier, inc=1, device_id=place(step), device_id_type=MESH)
        return carry

    lax.fori_loop(1, count, greet, 0)
    pl.semaphore_wait(barrier, count - 1)

    def table_copies(way):
        to = {"band": band - 1 if way == 0 else band + 1}
        pairs = ((tile_h, tile_in), (block_h, block_in), (live_h, live_in))
        return [
            pltpu.make_async_remote_copy(
                src_ref=mine,
                dst_ref=theirs.at[way],
                send_sem=table_send.at[way, i],
                recv_sem=table_recv.at[way, i],
                device_id=to,
                device_id_type=MESH,
            )
            for i, (mine, theirs) in enumerate(pairs)
        ]

    def edge_copy(way, j):
        return pltpu.make_async_remote_copy(
            src_ref=made.at[way, j],
            dst_ref=came.at[way, j],
            send_sem=edge_send.at[way, j],
            recv_sem=edge_recv.at[way, j],
            device_id={"band": band + 1 if way == 0 else band - 1},
            device_id_type=MESH,
        )

    for way, there in ((0, has_low), (1, has_high)):
        @pl.when(there)
        def _(way=way):
            for copy in table_copies(way):
                copy.start()

    held[tiles.shape[0]] = jnp.zeros((tile, tile), held.dtype)
    target_sum[...] = jnp.zeros_like(target_sum)

    def weigh(c, running):
        loads[c].wait()

        def one(n, running):
            at = pl.ds(pl.multiple_of(n * tile, tile), tile)
            scale = area[:, at] * mask[:, at].astype(jnp.float32)
            part = stage[:, :, at].astype(jnp.float32).reshape(columns, tile) * scale
            part = part.astype(source.dtype)
            source[n] = part
            return running + part.astype(jnp.float32)

        return lax.fori_loop(c * HALO_BLK, (c + 1) * HALO_BLK, one, running, unroll=4)

    source_sum = jnp.zeros((columns, tile), jnp.float32)
    small[0].wait()
    small[1].wait()
    for c in order[:2]:
        source_sum = weigh(c, source_sum)
    for copy in small[2:]:
        copy.wait()

    for way, there in ((0, has_high), (1, has_low)):
        @pl.when(there)
        def _(way=way):
            for copy in table_copies(way):
                copy.wait_recv()
            pairs = ((tile_in, tile_n), (block_in, block_n), (live_in, live_n))
            lists = [
                pltpu.make_async_copy(a.at[way], b.at[way], list_sem.at[way, i])
                for i, (a, b) in enumerate(pairs)
            ]
            for copy in lists:
                copy.start()
            for copy in lists:
                copy.wait()
            table = (
                lambda k, n: tile_n[way, k, n],
                lambda k, n: block_n[way, k, n],
                lambda n: live_n[way, 0, n],
            )
            first = 0 if way == 0 else targets - edge
            if way == 0:
                reach = (HALO_BLK - own, own - HALO_BLK, own)
            else:
                reach = (HALO_BLK + own, 0, HALO_BLK)

            def one(j, carry):
                value = slot_dot(source, held, table, first + j, slots, *reach)
                made[way, j] = value.astype(made.dtype)
                target_sum[...] += value

                @pl.when(j > 0)
                def _():
                    edge_copy(way, j - 1).start()

                return carry

            lax.fori_loop(0, edge, one, 0)

    for i, c in enumerate(order[2:]):
        source_sum = weigh(c, source_sum)
        if i == 0:
            for way, there in ((0, has_high), (1, has_low)):
                @pl.when(there)
                def _(way=way):
                    edge_copy(way, edge - 1).start()

    own_table = (
        lambda k, n: tile_s[k, n],
        lambda k, n: block_s[k, n],
        lambda n: live_s[0, n],
    )

    def own_group(g, carry):
        for u in range(OWN_UNROLL):
            t = g * OWN_UNROLL + u
            value = slot_dot(source, held, own_table, t, slots, HALO_BLK, 0, own)
            raw[t] = value
            carry = carry + value
        return carry

    target_total = lax.fori_loop(0, targets // OWN_UNROLL, own_group, target_sum[...])
    rows[0:1, :] = row_of(source_sum)
    rows[1:2, :] = row_of(target_total)
    rows[2:3, :] = jnp.broadcast_to(
        jnp.sum(target_area[...], axis=1, keepdims=True), (1, columns)
    )
    rows[3:8, :] = jnp.zeros((5, columns), jnp.float32)

    def divide(t, carry):
        at = pl.ds(pl.multiple_of(t * tile, tile), tile)
        raw[t] = raw[t] / target_area[:, at]
        return carry

    lax.fori_loop(edge, targets - edge, divide, 0, unroll=4)

    def row_copy(step):
        return pltpu.make_async_remote_copy(
            src_ref=rows,
            dst_ref=landed.at[step],
            send_sem=row_send.at[step],
            recv_sem=row_recv.at[step],
            device_id=place(step),
            device_id_type=MESH,
        )

    def begin(step, carry):
        row_copy(step).start()
        return carry

    def end(step, carry):
        row_copy(step).wait()
        return carry

    lax.fori_loop(1, count, begin, 0)
    landed[0] = rows[...]

    for way, there in ((0, has_low), (1, has_high)):
        @pl.when(there)
        def _(way=way):
            def add(j, carry):
                edge_copy(way, j).wait_recv()
                t = j if way == 0 else targets - edge + j
                raw[t] = raw[t] + came[way, j].astype(jnp.float32)
                return carry

            lax.fori_loop(0, edge, add, 0)

    lax.fori_loop(0, edge, divide, 0, unroll=4)
    lax.fori_loop(targets - edge, targets, divide, 0, unroll=4)

    for way, there in ((0, has_low), (1, has_high)):
        @pl.when(there)
        def _(way=way):
            for copy in table_copies(way):
                copy.wait_send()

    for way, there in ((0, has_high), (1, has_low)):
        @pl.when(there)
        def _(way=way):
            def sent(j, carry):
                edge_copy(way, j).wait_send()
                return carry

            lax.fori_loop(0, edge, sent, 0)

    lax.fori_loop(1, count, end, 0)
    for m in range(mems):
        total = jnp.zeros(rows.shape, jnp.float32)
        for b in range(bands):
            total = total + landed[lax.rem(me - (m * bands + b) + count, count)]
        totals[m] = total
    mine = totals[mem]
    fix = (mine[0:1, :] - mine[1:2, :]) / mine[2:3, :]
    fix_ref[...] = jnp.broadcast_to(fix, (fix_ref.shape[1], fix.shape[1])).T


def main_call(fields, mask, area, target_area, tiles, tile_t, block_t, live):
    bands, mems = lax.axis_size("band"), lax.axis_size("mem")
    rows, snaps, cells = fields.shape
    columns = rows * snaps
    slots, targets = tile_t.shape
    count, tile = tiles.shape[0], tiles.shape[1]
    own = cells // tile
    edge = HALO_BLK // (own // targets)
    dma = pltpu.SemaphoreType.DMA
    peers = bands * mems
    return pl.pallas_call(
        functools.partial(main_kernel, bands, mems, edge),
        in_specs=[HBM] * 8,
        out_specs=(VMEM, VMEM, VMEM),
        out_shape=(
            jax.ShapeDtypeStruct((targets, columns, tile), jnp.float32),
            jax.ShapeDtypeStruct((mems, 8, columns), jnp.float32),
            jax.ShapeDtypeStruct((columns, tile), jnp.float32),
        ),
        scratch_shapes=[
            pltpu.VMEM(mask.shape, mask.dtype),
            pltpu.VMEM(area.shape, area.dtype),
            pltpu.VMEM(target_area.shape, target_area.dtype),
            pltpu.SMEM(tile_t.shape, tile_t.dtype),
            pltpu.SMEM(block_t.shape, block_t.dtype),
            pltpu.SMEM(live.shape, live.dtype),
            pltpu.VMEM(fields.shape, fields.dtype),
            pltpu.VMEM((own, columns, tile), jnp.bfloat16),
            pltpu.VMEM((count + 1, tile, tile), tiles.dtype),
            pltpu.VMEM((2, edge, columns, tile), SEND_TYPE),
            pltpu.VMEM((2, edge, columns, tile), SEND_TYPE),
            pltpu.VMEM((8, columns), jnp.float32),
            pltpu.VMEM((peers, 8, columns), jnp.float32),
            pltpu.VMEM((columns, tile), jnp.float32),
            pltpu.VMEM((2, slots, targets), jnp.int32),
            pltpu.VMEM((2, slots, targets), jnp.int32),
            pltpu.VMEM((2, 1, targets), jnp.int32),
            pltpu.SMEM((2, slots, targets), jnp.int32),
            pltpu.SMEM((2, slots, targets), jnp.int32),
            pltpu.SMEM((2, 1, targets), jnp.int32),
            dma((own // HALO_BLK,)),
            dma((7,)),
            dma((2, 3)),
            dma((2, 3)),
            dma((2, 3)),
            dma((2, edge)),
            dma((2, edge)),
            dma((peers,)),
            dma((peers,)),
        ],
        compiler_params=pltpu.CompilerParams(
            collective_id=0, has_side_effects=True, vmem_limit_bytes=32 << 20
        ),
    )(fields, mask, area, target_area, tiles, tile_t, block_t, live)


def finish_kernel(fields, snaps, raw_ref, fix_ref, totals_ref, out_ref, mean_ref, ensemble_ref):
    count, columns, tile = raw_ref.shape
    fix = fix_ref[...]
    for n in range(count):
        value = raw_ref[n] + fix
        out_ref[:, :, n * tile:(n + 1) * tile] = value.reshape(columns // snaps, snaps, tile)

    @pl.when(pl.program_id(0) == 0)
    def _():
        mems, members = totals_ref.shape[0], mean_ref.shape[0]
        spot = lax.broadcasted_iota(jnp.int32, (columns, tile), 0)
        lane = lax.broadcasted_iota(jnp.int32, (columns, tile), 1)
        chosen = lax.rem(spot, snaps) == lane
        summed = jnp.zeros((fields, snaps), jnp.float32)

        def table(m):
            row = totals_ref[m, 0:1, :] / totals_ref[m, 2:3, :]
            column = jnp.broadcast_to(row, (tile, columns)).T
            spread = jnp.where(chosen, column, 0.0).reshape(columns // snaps, snaps, tile)
            return jnp.sum(spread, axis=1)[:, 0:snaps]

        mine = table(lax.axis_index("mem"))
        for n in range(members):
            mean_ref[n] = mine[n * fields:(n + 1) * fields]
        for m in range(mems):
            all_of = table(m)
            for n in range(members):
                summed = summed + all_of[n * fields:(n + 1) * fields]
        ensemble_ref[...] = summed / (mems * members)


def finish(raw, fix, totals, members, fields, snaps):
    targets, columns, tile = raw.shape
    steps = 4
    part = targets // steps
    rows = members * fields
    return pl.pallas_call(
        functools.partial(finish_kernel, fields, snaps),
        grid=(steps,),
        in_specs=[
            pl.BlockSpec((part, columns, tile), lambda i: (i, 0, 0)),
            pl.BlockSpec((columns, tile), lambda i: (0, 0)),
            pl.BlockSpec(totals.shape, lambda i: (0, 0, 0)),
        ],
        out_specs=(
            pl.BlockSpec((rows, snaps, part * tile), lambda i: (0, 0, i)),
            pl.BlockSpec((members, fields, snaps), lambda i: (0, 0, 0)),
            pl.BlockSpec((fields, snaps), lambda i: (0, 0)),
        ),
        out_shape=(
            jax.ShapeDtypeStruct((rows, snaps, targets * tile), jnp.float32),
            jax.ShapeDtypeStruct((members, fields, snaps), jnp.float32),
            jax.ShapeDtypeStruct((fields, snaps), jnp.float32),
        ),
        compiler_params=pltpu.CompilerParams(vmem_limit_bytes=16 << 20),
    )(raw, fix, totals)


def on_device(
    surface_fields, land_mask, source_area, target_area, weight_tiles, tile_of, block_of, live_slots
):
    members, fields, snaps, cells = surface_fields.shape
    targets = tile_of.shape[0]
    target_cells = target_area.shape[0]
    raw, totals, fix = main_call(
        surface_fields.reshape(members * fields, snaps, cells),
        land_mask.reshape(1, cells),
        source_area.reshape(1, cells),
        target_area.reshape(1, target_cells),
        weight_tiles,
        tile_of.T,
        block_of.T,
        live_slots.reshape(1, targets),
    )
    regridded, conserved, ensemble = finish(raw, fix, totals, members, fields, snaps)
    return regridded.reshape(members, fields, snaps, target_cells), conserved, ensemble


def solution(mesh):
    placed = (
        P(("grp", "mem"), "fld", None, "band"),
        P("band"),
        P("band"),
        P("band"),
        P(),
        P("band", None),
        P("band", None),
        P("band"),
    )
    return jax.shard_map(
        on_device,
        mesh=mesh,
        in_specs=placed,
        out_specs=(
            P(("grp", "mem"), "fld", None, "band"),
            P(("grp", "mem"), "fld", None),
            P(("grp", "fld"), None),
        ),
        check_vma=False,
    )
```

```python
import functools

import jax
import jax.numpy as jnp
from jax import lax
from jax.experimental import pallas as pl
from jax.experimental.pallas import tpu as pltpu
from jax.sharding import PartitionSpec as P

HALO_BLK = 32
OWN_UNROLL = 2
SEND_TYPE = jnp.float32
MESH = pl.DeviceIdType.MESH
HBM = pl.BlockSpec(memory_space=pltpu.HBM)
VMEM = pl.BlockSpec(memory_space=pltpu.VMEM)


def row_of(sums):
    return jnp.sum(sums.T, axis=0, keepdims=True)


def slot_dot(source, held, table, n, slots, shift, low, high):
    tiles, blocks, live = table
    used, zero_tile = live(n), held.shape[0] - 1
    left, right = [], []
    for k in range(slots):
        block = blocks(k, n) - shift
        keep = (k < used) & (block >= low) & (block < high)
        left.append(source[jnp.where(keep, block, low)])
        right.append(held[jnp.where(keep, tiles(k, n), zero_tile)])
    return jnp.dot(
        jnp.concatenate(left, axis=1),
        jnp.concatenate(right, axis=0),
        preferred_element_type=jnp.float32,
    )


def main_kernel(
    bands, mems, edge,
    fields, mask_h, area_h, target_area_h, tiles, tile_h, block_h, live_h,
    raw, totals, fix_ref,
    mask, area, target_area, tile_s, block_s, live_s,
    stage, source, held, made, came, rows, landed, target_sum,
    tile_in, block_in, live_in, tile_n, block_n, live_n,
    load_sem, small_sem, list_sem, table_send, table_recv, edge_send, edge_recv, row_send, row_recv,
):
    band, mem = lax.axis_index("band"), lax.axis_index("mem")
    count = bands * mems
    me = mem * bands + band
    own, columns, tile = source.shape
    slots, targets = tile_h.shape
    has_low, has_high = band > 0, band < bands - 1
    chunk = HALO_BLK * tile
    chunks = own // HALO_BLK
    order = [0, chunks - 1] + list(range(1, chunks - 1))

    loads = [
        pltpu.make_async_copy(
            fields.at[:, :, pl.ds(c * chunk, chunk)],
            stage.at[:, :, pl.ds(c * chunk, chunk)],
            load_sem.at[c],
        )
        for c in range(chunks)
    ]
    small = [
        pltpu.make_async_copy(a, b, small_sem.at[i])
        for i, (a, b) in enumerate((
            (mask_h, mask),
            (area_h, area),
            (tiles, held.at[pl.ds(0, tiles.shape[0])]),
            (tile_h, tile_s),
            (block_h, block_s),
            (live_h, live_s),
            (target_area_h, target_area),
        ))
    ]
    small[0].start()
    small[1].start()
    for c in order[:2]:
        loads[c].start()
    for copy in small[2:]:
        copy.start()
    for c in order[2:]:
        loads[c].start()

    def place(step):
        other = lax.rem(me + step, count)
        return {"mem": other // bands, "band": lax.rem(other, bands)}

    barrier = pltpu.get_barrier_semaphore()

    def greet(step, carry):
        pl.semaphore_signal(barrier, inc=1, device_id=place(step), device_id_type=MESH)
        return carry

    lax.fori_loop(1, count, greet, 0)
    pl.semaphore_wait(barrier, count - 1)

    def table_copies(way):
        to = {"band": band - 1 if way == 0 else band + 1}
        pairs = ((tile_h, tile_in), (block_h, block_in), (live_h, live_in))
        return [
            pltpu.make_async_remote_copy(
                src_ref=mine,
                dst_ref=theirs.at[way],
                send_sem=table_send.at[way, i],
                recv_sem=table_recv.at[way, i],
                device_id=to,
                device_id_type=MESH,
            )
            for i, (mine, theirs) in enumerate(pairs)
        ]

    def edge_copy(way, j):
        return pltpu.make_async_remote_copy(
            src_ref=made.at[way, j],
            dst_ref=came.at[way, j],
            send_sem=edge_send.at[way, j],
            recv_sem=edge_recv.at[way, j],
            device_id={"band": band + 1 if way == 0 else band - 1},
            device_id_type=MESH,
        )

    for way, there in ((0, has_low), (1, has_high)):
        @pl.when(there)
        def _(way=way):
            for copy in table_copies(way):
                copy.start()

    held[tiles.shape[0]] = jnp.zeros((tile, tile), held.dtype)
    target_sum[...] = jnp.zeros_like(target_sum)

    def weigh(c, running):
        loads[c].wait()

        def one(n, running):
            at = pl.ds(pl.multiple_of(n * tile, tile), tile)
            scale = area[:, at] * mask[:, at].astype(jnp.float32)
            part = stage[:, :, at].astype(jnp.float32).reshape(columns, tile) * scale
            part = part.astype(source.dtype)
            source[n] = part
            return running + part.astype(jnp.float32)

        return lax.fori_loop(c * HALO_BLK, (c + 1) * HALO_BLK, one, running, unroll=4)

    source_sum = jnp.zeros((columns, tile), jnp.float32)
    small[0].wait()
    small[1].wait()
    for c in order[:2]:
        source_sum = weigh(c, source_sum)
    for copy in small[2:]:
        copy.wait()

    for way, there in ((0, has_high), (1, has_low)):
        @pl.when(there)
        def _(way=way):
            for copy in table_copies(way):
                copy.wait_recv()
            pairs = ((tile_in, tile_n), (block_in, block_n), (live_in, live_n))
            lists = [
                pltpu.make_async_copy(a.at[way], b.at[way], list_sem.at[way, i])
                for i, (a, b) in enumerate(pairs)
            ]
            for copy in lists:
                copy.start()
            for copy in lists:
                copy.wait()
            table = (
                lambda k, n: tile_n[way, k, n],
                lambda k, n: block_n[way, k, n],
                lambda n: live_n[way, 0, n],
            )
            first = 0 if way == 0 else targets - edge
            if way == 0:
                reach = (HALO_BLK - own, own - HALO_BLK, own)
            else:
                reach = (HALO_BLK + own, 0, HALO_BLK)

            def one(j, carry):
                value = slot_dot(source, held, table, first + j, slots, *reach)
                made[way, j] = value.astype(made.dtype)
                target_sum[...] += value

                @pl.when(j > 0)
                def _():
                    edge_copy(way, j - 1).start()

                return carry

            lax.fori_loop(0, edge, one, 0)

    for i, c in enumerate(order[2:]):
        source_sum = weigh(c, source_sum)
        if i == 0:
            for way, there in ((0, has_high), (1, has_low)):
                @pl.when(there)
                def _(way=way):
                    edge_copy(way, edge - 1).start()

    own_table = (
        lambda k, n: tile_s[k, n],
        lambda k, n: block_s[k, n],
        lambda n: live_s[0, n],
    )

    def own_group(g, carry):
        for u in range(OWN_UNROLL):
            t = g * OWN_UNROLL + u
            value = slot_dot(source, held, own_table, t, slots, HALO_BLK, 0, own)
            raw[t] = value
            carry = carry + value
        return carry

    target_total = lax.fori_loop(0, targets // OWN_UNROLL, own_group, target_sum[...])
    rows[0:1, :] = row_of(source_sum)
    rows[1:2, :] = row_of(target_total)
    rows[2:3, :] = jnp.broadcast_to(
        jnp.sum(target_area[...], axis=1, keepdims=True), (1, columns)
    )
    rows[3:8, :] = jnp.zeros((5, columns), jnp.float32)

    def divide(t, carry):
        at = pl.ds(pl.multiple_of(t * tile, tile), tile)
        raw[t] = raw[t] / target_area[:, at]
        return carry

    lax.fori_loop(edge, targets - edge, divide, 0, unroll=4)

    def row_copy(step):
        return pltpu.make_async_remote_copy(
            src_ref=rows,
            dst_ref=landed.at[step],
            send_sem=row_send.at[step],
            recv_sem=row_recv.at[step],
            device_id=place(step),
            device_id_type=MESH,
        )

    def begin(step, carry):
        row_copy(step).start()
        return carry

    def end(step, carry):
        row_copy(step).wait()
        return carry

    lax.fori_loop(1, count, begin, 0)
    landed[0] = rows[...]

    for way, there in ((0, has_low), (1, has_high)):
        @pl.when(there)
        def _(way=way):
            def add(j, carry):
                edge_copy(way, j).wait_recv()
                t = j if way == 0 else targets - edge + j
                raw[t] = raw[t] + came[way, j].astype(jnp.float32)
                return carry

            lax.fori_loop(0, edge, add, 0)

    lax.fori_loop(0, edge, divide, 0, unroll=4)
    lax.fori_loop(targets - edge, targets, divide, 0, unroll=4)

    for way, there in ((0, has_low), (1, has_high)):
        @pl.when(there)
        def _(way=way):
            for copy in table_copies(way):
                copy.wait_send()

    for way, there in ((0, has_high), (1, has_low)):
        @pl.when(there)
        def _(way=way):
            def sent(j, carry):
                edge_copy(way, j).wait_send()
                return carry

            lax.fori_loop(0, edge, sent, 0)

    lax.fori_loop(1, count, end, 0)
    for m in range(mems):
        total = jnp.zeros(rows.shape, jnp.float32)
        for b in range(bands):
            total = total + landed[lax.rem(me - (m * bands + b) + count, count)]
        totals[m] = total
    mine = totals[mem]
    fix = (mine[0:1, :] - mine[1:2, :]) / mine[2:3, :]
    fix_ref[...] = jnp.broadcast_to(fix, (fix_ref.shape[1], fix.shape[1])).T


def main_call(fields, mask, area, target_area, tiles, tile_t, block_t, live):
    bands, mems = lax.axis_size("band"), lax.axis_size("mem")
    rows, snaps, cells = fields.shape
    columns = rows * snaps
    slots, targets = tile_t.shape
    count, tile = tiles.shape[0], tiles.shape[1]
    own = cells // tile
    edge = HALO_BLK // (own // targets)
    dma = pltpu.SemaphoreType.DMA
    peers = bands * mems
    return pl.pallas_call(
        functools.partial(main_kernel, bands, mems, edge),
        in_specs=[HBM] * 8,
        out_specs=(VMEM, VMEM, VMEM),
        out_shape=(
            jax.ShapeDtypeStruct((targets, columns, tile), jnp.float32),
            jax.ShapeDtypeStruct((mems, 8, columns), jnp.float32),
            jax.ShapeDtypeStruct((columns, tile), jnp.float32),
        ),
        scratch_shapes=[
            pltpu.VMEM(mask.shape, mask.dtype),
            pltpu.VMEM(area.shape, area.dtype),
            pltpu.VMEM(target_area.shape, target_area.dtype),
            pltpu.SMEM(tile_t.shape, tile_t.dtype),
            pltpu.SMEM(block_t.shape, block_t.dtype),
            pltpu.SMEM(live.shape, live.dtype),
            pltpu.VMEM(fields.shape, fields.dtype),
            pltpu.VMEM((own, columns, tile), jnp.bfloat16),
            pltpu.VMEM((count + 1, tile, tile), tiles.dtype),
            pltpu.VMEM((2, edge, columns, tile), SEND_TYPE),
            pltpu.VMEM((2, edge, columns, tile), SEND_TYPE),
            pltpu.VMEM((8, columns), jnp.float32),
            pltpu.VMEM((peers, 8, columns), jnp.float32),
            pltpu.VMEM((columns, tile), jnp.float32),
            pltpu.VMEM((2, slots, targets), jnp.int32),
            pltpu.VMEM((2, slots, targets), jnp.int32),
            pltpu.VMEM((2, 1, targets), jnp.int32),
            pltpu.SMEM((2, slots, targets), jnp.int32),
            pltpu.SMEM((2, slots, targets), jnp.int32),
            pltpu.SMEM((2, 1, targets), jnp.int32),
            dma((own // HALO_BLK,)),
            dma((7,)),
            dma((2, 3)),
            dma((2, 3)),
            dma((2, 3)),
            dma((2, edge)),
            dma((2, edge)),
            dma((peers,)),
            dma((peers,)),
        ],
        compiler_params=pltpu.CompilerParams(
            collective_id=0, has_side_effects=True, vmem_limit_bytes=32 << 20
        ),
    )(*[pltpu.with_memory_space_constraint(a, pltpu.HBM) for a in (fields, mask, area, target_area, tiles, tile_t, block_t, live)])


def finish_kernel(fields, snaps, raw_ref, fix_ref, totals_ref, out_ref, mean_ref, ensemble_ref):
    count, columns, tile = raw_ref.shape
    fix = fix_ref[...]
    for n in range(count):
        value = raw_ref[n] + fix
        out_ref[:, :, n * tile:(n + 1) * tile] = value.reshape(columns // snaps, snaps, tile)

    @pl.when(pl.program_id(0) == 0)
    def _():
        mems, members = totals_ref.shape[0], mean_ref.shape[0]
        spot = lax.broadcasted_iota(jnp.int32, (columns, tile), 0)
        lane = lax.broadcasted_iota(jnp.int32, (columns, tile), 1)
        chosen = lax.rem(spot, snaps) == lane
        summed = jnp.zeros((fields, snaps), jnp.float32)

        def table(m):
            row = totals_ref[m, 0:1, :] / totals_ref[m, 2:3, :]
            column = jnp.broadcast_to(row, (tile, columns)).T
            spread = jnp.where(chosen, column, 0.0).reshape(columns // snaps, snaps, tile)
            return jnp.sum(spread, axis=1)[:, 0:snaps]

        mine = table(lax.axis_index("mem"))
        for n in range(members):
            mean_ref[n] = mine[n * fields:(n + 1) * fields]
        for m in range(mems):
            all_of = table(m)
            for n in range(members):
                summed = summed + all_of[n * fields:(n + 1) * fields]
        ensemble_ref[...] = summed / (mems * members)


def finish(raw, fix, totals, members, fields, snaps):
    targets, columns, tile = raw.shape
    steps = 4
    part = targets // steps
    rows = members * fields
    return pl.pallas_call(
        functools.partial(finish_kernel, fields, snaps),
        grid=(steps,),
        in_specs=[
            pl.BlockSpec((part, columns, tile), lambda i: (i, 0, 0)),
            pl.BlockSpec((columns, tile), lambda i: (0, 0)),
            pl.BlockSpec(totals.shape, lambda i: (0, 0, 0)),
        ],
        out_specs=(
            pl.BlockSpec((rows, snaps, part * tile), lambda i: (0, 0, i)),
            pl.BlockSpec((members, fields, snaps), lambda i: (0, 0, 0)),
            pl.BlockSpec((fields, snaps), lambda i: (0, 0)),
        ),
        out_shape=(
            jax.ShapeDtypeStruct((rows, snaps, targets * tile), jnp.float32),
            jax.ShapeDtypeStruct((members, fields, snaps), jnp.float32),
            jax.ShapeDtypeStruct((fields, snaps), jnp.float32),
        ),
        compiler_params=pltpu.CompilerParams(vmem_limit_bytes=16 << 20),
    )(raw, fix, totals)


def on_device(
    surface_fields, land_mask, source_area, target_area, weight_tiles, tile_of, block_of, live_slots
):
    members, fields, snaps, cells = surface_fields.shape
    targets = tile_of.shape[0]
    target_cells = target_area.shape[0]
    raw, totals, fix = main_call(
        surface_fields.reshape(members * fields, snaps, cells),
        land_mask.reshape(1, cells),
        source_area.reshape(1, cells),
        target_area.reshape(1, target_cells),
        weight_tiles,
        tile_of.T,
        block_of.T,
        live_slots.reshape(1, targets),
    )
    regridded, conserved, ensemble = finish(raw, fix, totals, members, fields, snaps)
    return regridded.reshape(members, fields, snaps, target_cells), conserved, ensemble


def solution(mesh):
    placed = (
        P(("grp", "mem"), "fld", None, "band"),
        P("band"),
        P("band"),
        P("band"),
        P(),
        P("band", None),
        P("band", None),
        P("band"),
    )
    return jax.shard_map(
        on_device,
        mesh=mesh,
        in_specs=placed,
        out_specs=(
            P(("grp", "mem"), "fld", None, "band"),
            P(("grp", "mem"), "fld", None),
            P(("grp", "fld"), None),
        ),
        check_vma=False,
    )
```

```python
import functools

import jax
import jax.numpy as jnp
from jax import lax
from jax.experimental import pallas as pl
from jax.experimental.pallas import tpu as pltpu
from jax.sharding import PartitionSpec as P

HALO_BLK = 32
OWN_UNROLL = 4
SEND_TYPE = jnp.float32
MESH = pl.DeviceIdType.MESH
HBM = pl.BlockSpec(memory_space=pltpu.HBM)
VMEM = pl.BlockSpec(memory_space=pltpu.VMEM)


def row_of(sums):
    return jnp.sum(sums.T, axis=0, keepdims=True)


def slot_dot(source, held, table, n, slots, shift, low, high):
    tiles, blocks, live = table
    used, zero_tile = live(n), held.shape[0] - 1
    left, right = [], []
    for k in range(slots):
        block = blocks(k, n) - shift
        keep = (k < used) & (block >= low) & (block < high)
        left.append(source[jnp.where(keep, block, low)])
        right.append(held[jnp.where(keep, tiles(k, n), zero_tile)])
    return jnp.dot(
        jnp.concatenate(left, axis=1),
        jnp.concatenate(right, axis=0),
        preferred_element_type=jnp.float32,
    )


def main_kernel(
    bands, mems, edge,
    fields, mask_h, area_h, target_area_h, tiles, tile_h, block_h, live_h,
    raw, totals, fix_ref,
    mask, area, target_area, tile_s, block_s, live_s,
    stage, source, held, made, came, rows, landed, target_sum,
    tile_in, block_in, live_in, tile_n, block_n, live_n,
    load_sem, small_sem, list_sem, table_send, table_recv, edge_send, edge_recv, row_send, row_recv,
):
    band, mem = lax.axis_index("band"), lax.axis_index("mem")
    count = bands * mems
    me = mem * bands + band
    own, columns, tile = source.shape
    slots, targets = tile_h.shape
    has_low, has_high = band > 0, band < bands - 1
    chunk = HALO_BLK * tile
    chunks = own // HALO_BLK
    order = [0, chunks - 1] + list(range(1, chunks - 1))

    loads = [
        pltpu.make_async_copy(
            fields.at[:, :, pl.ds(c * chunk, chunk)],
            stage.at[:, :, pl.ds(c * chunk, chunk)],
            load_sem.at[c],
        )
        for c in range(chunks)
    ]
    small = [
        pltpu.make_async_copy(a, b, small_sem.at[i])
        for i, (a, b) in enumerate((
            (mask_h, mask),
            (area_h, area),
            (tiles, held.at[pl.ds(0, tiles.shape[0])]),
            (tile_h, tile_s),
            (block_h, block_s),
            (live_h, live_s),
            (target_area_h, target_area),
        ))
    ]
    small[0].start()
    small[1].start()
    for c in order[:2]:
        loads[c].start()
    for copy in small[2:]:
        copy.start()
    for c in order[2:]:
        loads[c].start()

    def place(step):
        other = lax.rem(me + step, count)
        return {"mem": other // bands, "band": lax.rem(other, bands)}

    barrier = pltpu.get_barrier_semaphore()

    def greet(step, carry):
        pl.semaphore_signal(barrier, inc=1, device_id=place(step), device_id_type=MESH)
        return carry

    lax.fori_loop(1, count, greet, 0)
    pl.semaphore_wait(barrier, count - 1)

    def table_copies(way):
        to = {"band": band - 1 if way == 0 else band + 1}
        pairs = ((tile_h, tile_in), (block_h, block_in), (live_h, live_in))
        return [
            pltpu.make_async_remote_copy(
                src_ref=mine,
                dst_ref=theirs.at[way],
                send_sem=table_send.at[way, i],
                recv_sem=table_recv.at[way, i],
                device_id=to,
                device_id_type=MESH,
            )
            for i, (mine, theirs) in enumerate(pairs)
        ]

    def edge_copy(way, j):
        return pltpu.make_async_remote_copy(
            src_ref=made.at[way, j],
            dst_ref=came.at[way, j],
            send_sem=edge_send.at[way, j],
            recv_sem=edge_recv.at[way, j],
            device_id={"band": band + 1 if way == 0 else band - 1},
            device_id_type=MESH,
        )

    for way, there in ((0, has_low), (1, has_high)):
        @pl.when(there)
        def _(way=way):
            for copy in table_copies(way):
                copy.start()

    held[tiles.shape[0]] = jnp.zeros((tile, tile), held.dtype)

    def fetch(pairs):
        copies = [
            pltpu.make_async_copy(a, b, list_sem.at[i]) for i, (a, b) in enumerate(pairs)
        ]
        for copy in copies:
            copy.start()
        for copy in copies:
            copy.wait()

    def weigh(c, running):
        loads[c].wait()

        def one(n, running):
            at = pl.ds(pl.multiple_of(n * tile, tile), tile)
            scale = area[:, at] * mask[:, at].astype(jnp.float32)
            part = stage[:, :, at].astype(jnp.float32).reshape(columns, tile) * scale
            part = part.astype(source.dtype)
            source[n] = part
            return running + part.astype(jnp.float32)

        return lax.fori_loop(c * HALO_BLK, (c + 1) * HALO_BLK, one, running, unroll=4)

    source_sum = jnp.zeros((columns, tile), jnp.float32)
    small[0].wait()
    small[1].wait()
    for c in order[:2]:
        source_sum = weigh(c, source_sum)
    for copy in small[2:]:
        copy.wait()

    for way, there in ((0, has_high), (1, has_low)):
        @pl.when(there)
        def _(way=way):
            for copy in table_copies(way):
                copy.wait_recv()
            pairs = ((tile_in, tile_n), (block_in, block_n), (live_in, live_n))
            fetch([(a.at[way], b.at[way]) for a, b in pairs])

        @pl.when(jnp.logical_not(there))
        def _(way=way):
            pairs = ((tile_h, tile_n), (block_h, block_n), (live_h, live_n))
            fetch([(a, b.at[way]) for a, b in pairs])

    reaches = (
        (HALO_BLK - own, own - HALO_BLK, own),
        (HALO_BLK + own, 0, HALO_BLK),
    )

    def one_edge(j, carry):
        for way, there in ((0, has_high), (1, has_low)):
            table = (
                lambda k, n, way=way: tile_n[way, k, n],
                lambda k, n, way=way: block_n[way, k, n],
                lambda n, way=way: live_n[way, 0, n],
            )
            first = 0 if way == 0 else targets - edge
            value = slot_dot(source, held, table, first + j, slots, *reaches[way])
            made[way, j] = value.astype(made.dtype)
            carry = carry + value * there.astype(jnp.float32)

        for way, there in ((0, has_high), (1, has_low)):
            @pl.when((j > 0) & there)
            def _(way=way):
                edge_copy(way, j - 1).start()

        return carry

    edge_total = lax.fori_loop(0, edge, one_edge, jnp.zeros((columns, tile), jnp.float32))
    target_sum[...] = edge_total

    for i, c in enumerate(order[2:]):
        source_sum = weigh(c, source_sum)
        if i == 0:
            for way, there in ((0, has_high), (1, has_low)):
                @pl.when(there)
                def _(way=way):
                    edge_copy(way, edge - 1).start()

    own_table = (
        lambda k, n: tile_s[k, n],
        lambda k, n: block_s[k, n],
        lambda n: live_s[0, n],
    )

    def own_group(g, carry):
        for u in range(OWN_UNROLL):
            t = g * OWN_UNROLL + u
            value = slot_dot(source, held, own_table, t, slots, HALO_BLK, 0, own)
            raw[t] = value
            carry = carry + value
        return carry

    target_total = lax.fori_loop(0, targets // OWN_UNROLL, own_group, target_sum[...])
    rows[0:1, :] = row_of(source_sum)
    rows[1:2, :] = row_of(target_total)
    rows[2:3, :] = jnp.broadcast_to(
        jnp.sum(target_area[...], axis=1, keepdims=True), (1, columns)
    )
    rows[3:8, :] = jnp.zeros((5, columns), jnp.float32)

    def divide(t, carry):
        at = pl.ds(pl.multiple_of(t * tile, tile), tile)
        raw[t] = raw[t] / target_area[:, at]
        return carry

    lax.fori_loop(edge, targets - edge, divide, 0, unroll=4)

    def row_copy(step):
        return pltpu.make_async_remote_copy(
            src_ref=rows,
            dst_ref=landed.at[step],
            send_sem=row_send.at[step],
            recv_sem=row_recv.at[step],
            device_id=place(step),
            device_id_type=MESH,
        )

    def begin(step, carry):
        row_copy(step).start()
        return carry

    def end(step, carry):
        row_copy(step).wait()
        return carry

    lax.fori_loop(1, count, begin, 0)
    landed[0] = rows[...]

    for way, there in ((0, has_low), (1, has_high)):
        @pl.when(there)
        def _(way=way):
            def add(j, carry):
                edge_copy(way, j).wait_recv()
                t = j if way == 0 else targets - edge + j
                raw[t] = raw[t] + came[way, j].astype(jnp.float32)
                return carry

            lax.fori_loop(0, edge, add, 0)

    lax.fori_loop(0, edge, divide, 0, unroll=4)
    lax.fori_loop(targets - edge, targets, divide, 0, unroll=4)

    for way, there in ((0, has_low), (1, has_high)):
        @pl.when(there)
        def _(way=way):
            for copy in table_copies(way):
                copy.wait_send()

    for way, there in ((0, has_high), (1, has_low)):
        @pl.when(there)
        def _(way=way):
            def sent(j, carry):
                edge_copy(way, j).wait_send()
                return carry

            lax.fori_loop(0, edge, sent, 0)

    lax.fori_loop(1, count, end, 0)
    for m in range(mems):
        total = jnp.zeros(rows.shape, jnp.float32)
        for b in range(bands):
            total = total + landed[lax.rem(me - (m * bands + b) + count, count)]
        totals[m] = total
    mine = totals[mem]
    fix = (mine[0:1, :] - mine[1:2, :]) / mine[2:3, :]
    fix_ref[...] = jnp.broadcast_to(fix, (fix_ref.shape[1], fix.shape[1])).T


def main_call(fields, mask, area, target_area, tiles, tile_t, block_t, live):
    bands, mems = lax.axis_size("band"), lax.axis_size("mem")
    rows, snaps, cells = fields.shape
    columns = rows * snaps
    slots, targets = tile_t.shape
    count, tile = tiles.shape[0], tiles.shape[1]
    own = cells // tile
    edge = HALO_BLK // (own // targets)
    dma = pltpu.SemaphoreType.DMA
    peers = bands * mems
    return pl.pallas_call(
        functools.partial(main_kernel, bands, mems, edge),
        in_specs=[HBM] * 8,
        out_specs=(VMEM, VMEM, VMEM),
        out_shape=(
            jax.ShapeDtypeStruct((targets, columns, tile), jnp.float32),
            jax.ShapeDtypeStruct((mems, 8, columns), jnp.float32),
            jax.ShapeDtypeStruct((columns, tile), jnp.float32),
        ),
        scratch_shapes=[
            pltpu.VMEM(mask.shape, mask.dtype),
            pltpu.VMEM(area.shape, area.dtype),
            pltpu.VMEM(target_area.shape, target_area.dtype),
            pltpu.SMEM(tile_t.shape, tile_t.dtype),
            pltpu.SMEM(block_t.shape, block_t.dtype),
            pltpu.SMEM(live.shape, live.dtype),
            pltpu.VMEM(fields.shape, fields.dtype),
            pltpu.VMEM((own, columns, tile), jnp.bfloat16),
            pltpu.VMEM((count + 1, tile, tile), tiles.dtype),
            pltpu.VMEM((2, edge, columns, tile), SEND_TYPE),
            pltpu.VMEM((2, edge, columns, tile), SEND_TYPE),
            pltpu.VMEM((8, columns), jnp.float32),
            pltpu.VMEM((peers, 8, columns), jnp.float32),
            pltpu.VMEM((columns, tile), jnp.float32),
            pltpu.VMEM((2, slots, targets), jnp.int32),
            pltpu.VMEM((2, slots, targets), jnp.int32),
            pltpu.VMEM((2, 1, targets), jnp.int32),
            pltpu.SMEM((2, slots, targets), jnp.int32),
            pltpu.SMEM((2, slots, targets), jnp.int32),
            pltpu.SMEM((2, 1, targets), jnp.int32),
            dma((own // HALO_BLK,)),
            dma((7,)),
            dma((3,)),
            dma((2, 3)),
            dma((2, 3)),
            dma((2, edge)),
            dma((2, edge)),
            dma((peers,)),
            dma((peers,)),
        ],
        compiler_params=pltpu.CompilerParams(
            collective_id=0, has_side_effects=True, vmem_limit_bytes=32 << 20
        ),
    )(*[pltpu.with_memory_space_constraint(a, pltpu.HBM) for a in (fields, mask, area, target_area, tiles, tile_t, block_t, live)])


def finish_kernel(fields, snaps, raw_ref, fix_ref, totals_ref, out_ref, mean_ref, ensemble_ref):
    count, columns, tile = raw_ref.shape
    fix = fix_ref[...]
    for n in range(count):
        value = raw_ref[n] + fix
        out_ref[:, :, n * tile:(n + 1) * tile] = value.reshape(columns // snaps, snaps, tile)

    @pl.when(pl.program_id(0) == 0)
    def _():
        mems, members = totals_ref.shape[0], mean_ref.shape[0]
        spot = lax.broadcasted_iota(jnp.int32, (columns, tile), 0)
        lane = lax.broadcasted_iota(jnp.int32, (columns, tile), 1)
        chosen = lax.rem(spot, snaps) == lane
        summed = jnp.zeros((fields, snaps), jnp.float32)

        def table(m):
            row = totals_ref[m, 0:1, :] / totals_ref[m, 2:3, :]
            column = jnp.broadcast_to(row, (tile, columns)).T
            spread = jnp.where(chosen, column, 0.0).reshape(columns // snaps, snaps, tile)
            return jnp.sum(spread, axis=1)[:, 0:snaps]

        mine = table(lax.axis_index("mem"))
        for n in range(members):
            mean_ref[n] = mine[n * fields:(n + 1) * fields]
        for m in range(mems):
            all_of = table(m)
            for n in range(members):
                summed = summed + all_of[n * fields:(n + 1) * fields]
        ensemble_ref[...] = summed / (mems * members)


def finish(raw, fix, totals, members, fields, snaps):
    targets, columns, tile = raw.shape
    steps = 4
    part = targets // steps
    rows = members * fields
    return pl.pallas_call(
        functools.partial(finish_kernel, fields, snaps),
        grid=(steps,),
        in_specs=[
            pl.BlockSpec((part, columns, tile), lambda i: (i, 0, 0)),
            pl.BlockSpec((columns, tile), lambda i: (0, 0)),
            pl.BlockSpec(totals.shape, lambda i: (0, 0, 0)),
        ],
        out_specs=(
            pl.BlockSpec((rows, snaps, part * tile), lambda i: (0, 0, i)),
            pl.BlockSpec((members, fields, snaps), lambda i: (0, 0, 0)),
            pl.BlockSpec((fields, snaps), lambda i: (0, 0)),
        ),
        out_shape=(
            jax.ShapeDtypeStruct((rows, snaps, targets * tile), jnp.float32),
            jax.ShapeDtypeStruct((members, fields, snaps), jnp.float32),
            jax.ShapeDtypeStruct((fields, snaps), jnp.float32),
        ),
        compiler_params=pltpu.CompilerParams(vmem_limit_bytes=16 << 20),
    )(raw, fix, totals)


def on_device(
    surface_fields, land_mask, source_area, target_area, weight_tiles, tile_of, block_of, live_slots
):
    members, fields, snaps, cells = surface_fields.shape
    targets = tile_of.shape[0]
    target_cells = target_area.shape[0]
    raw, totals, fix = main_call(
        surface_fields.reshape(members * fields, snaps, cells),
        land_mask.reshape(1, cells),
        source_area.reshape(1, cells),
        target_area.reshape(1, target_cells),
        weight_tiles,
        tile_of.T,
        block_of.T,
        live_slots.reshape(1, targets),
    )
    regridded, conserved, ensemble = finish(raw, fix, totals, members, fields, snaps)
    return regridded.reshape(members, fields, snaps, target_cells), conserved, ensemble


def solution(mesh):
    placed = (
        P(("grp", "mem"), "fld", None, "band"),
        P("band"),
        P("band"),
        P("band"),
        P(),
        P("band", None),
        P("band", None),
        P("band"),
    )
    return jax.shard_map(
        on_device,
        mesh=mesh,
        in_specs=placed,
        out_specs=(
            P(("grp", "mem"), "fld", None, "band"),
            P(("grp", "mem"), "fld", None),
            P(("grp", "fld"), None),
        ),
        check_vma=False,
    )
```

```python
import functools

import jax
import jax.numpy as jnp
from jax import lax
from jax.experimental import pallas as pl
from jax.experimental.pallas import tpu as pltpu
from jax.sharding import PartitionSpec as P

HALO_BLK = 32
SEND_TYPE = jnp.float32
MESH = pl.DeviceIdType.MESH
HBM = pl.BlockSpec(memory_space=pltpu.HBM)
VMEM = pl.BlockSpec(memory_space=pltpu.VMEM)


def row_of(sums):
    return jnp.sum(sums.T, axis=0, keepdims=True)


def slot_dot(source, held, table, n, slots, shift, low, high):
    tiles, blocks, live = table
    used, zero_tile = live(n), held.shape[0] - 1
    left, right = [], []
    for k in range(slots):
        block = blocks(k, n) - shift
        keep = (k < used) & (block >= low) & (block < high)
        left.append(source[jnp.where(keep, block, low)])
        right.append(held[jnp.where(keep, tiles(k, n), zero_tile)])
    return jnp.dot(
        jnp.concatenate(left, axis=1),
        jnp.concatenate(right, axis=0),
        preferred_element_type=jnp.float32,
    )


def main_kernel(
    bands, mems, edge,
    fields, mask_h, area_h, target_area_h, tiles, tile_h, block_h, live_h,
    raw, totals, fix_ref,
    mask, area, target_area, tile_s, block_s, live_s,
    stage, source, held, made, came, rows, landed, target_sum,
    tile_in, block_in, live_in, tile_n, block_n, live_n,
    load_sem, small_sem, list_sem, table_send, table_recv, edge_send, edge_recv, row_send, row_recv,
):
    band, mem = lax.axis_index("band"), lax.axis_index("mem")
    count = bands * mems
    me = mem * bands + band
    own, columns, tile = source.shape
    slots, targets = tile_h.shape
    has_low, has_high = band > 0, band < bands - 1
    chunk = HALO_BLK * tile
    chunks = own // HALO_BLK
    order = [0, chunks - 1] + list(range(1, chunks - 1))

    def place(step):
        other = lax.rem(me + step, count)
        return {"mem": other // bands, "band": lax.rem(other, bands)}

    barrier = pltpu.get_barrier_semaphore()

    def greet(step, carry):
        pl.semaphore_signal(barrier, inc=1, device_id=place(step), device_id_type=MESH)
        return carry

    lax.fori_loop(1, count, greet, 0)

    loads = [
        pltpu.make_async_copy(
            fields.at[:, :, pl.ds(c * chunk, chunk)],
            stage.at[:, :, pl.ds(c * chunk, chunk)],
            load_sem.at[c],
        )
        for c in range(chunks)
    ]
    small = [
        pltpu.make_async_copy(a, b, small_sem.at[i])
        for i, (a, b) in enumerate((
            (mask_h, mask),
            (area_h, area),
            (tiles, held.at[pl.ds(0, tiles.shape[0])]),
            (tile_h, tile_s),
            (block_h, block_s),
            (live_h, live_s),
            (target_area_h, target_area),
        ))
    ]
    small[0].start()
    small[1].start()
    for c in order[:2]:
        loads[c].start()
    for copy in small[2:]:
        copy.start()
    for c in order[2:]:
        loads[c].start()

    pl.semaphore_wait(barrier, count - 1)

    def table_copies(way):
        to = {"band": band - 1 if way == 0 else band + 1}
        pairs = ((tile_h, tile_in), (block_h, block_in), (live_h, live_in))
        return [
            pltpu.make_async_remote_copy(
                src_ref=mine,
                dst_ref=theirs.at[way],
                send_sem=table_send.at[way, i],
                recv_sem=table_recv.at[way, i],
                device_id=to,
                device_id_type=MESH,
            )
            for i, (mine, theirs) in enumerate(pairs)
        ]

    def edge_copy(way, j):
        return pltpu.make_async_remote_copy(
            src_ref=made.at[way, j],
            dst_ref=came.at[way, j],
            send_sem=edge_send.at[way, j],
            recv_sem=edge_recv.at[way, j],
            device_id={"band": band + 1 if way == 0 else band - 1},
            device_id_type=MESH,
        )

    for way, there in ((0, has_low), (1, has_high)):
        @pl.when(there)
        def _(way=way):
            for copy in table_copies(way):
                copy.start()

    held[tiles.shape[0]] = jnp.zeros((tile, tile), held.dtype)

    def fetch(pairs):
        copies = [
            pltpu.make_async_copy(a, b, list_sem.at[i]) for i, (a, b) in enumerate(pairs)
        ]
        for copy in copies:
            copy.start()
        for copy in copies:
            copy.wait()

    def weigh(c, running):
        loads[c].wait()

        def one(n, running):
            at = pl.ds(pl.multiple_of(n * tile, tile), tile)
            scale = area[:, at] * mask[:, at].astype(jnp.float32)
            part = stage[:, :, at].astype(jnp.float32).reshape(columns, tile) * scale
            part = part.astype(source.dtype)
            source[n] = part
            return running + part.astype(jnp.float32)

        return lax.fori_loop(c * HALO_BLK, (c + 1) * HALO_BLK, one, running, unroll=4)

    source_sum = jnp.zeros((columns, tile), jnp.float32)
    small[0].wait()
    small[1].wait()
    for c in order:
        source_sum = weigh(c, source_sum)

    own_table = (
        lambda k, n: tile_s[k, n],
        lambda k, n: block_s[k, n],
        lambda n: live_s[0, n],
    )

    def own_group(first, width, carry):
        for u in range(width):
            t = first + u
            at = pl.ds(pl.multiple_of(t * tile, tile), tile)
            value = slot_dot(source, held, own_table, t, slots, HALO_BLK, 0, own)
            raw[t] = value * (1.0 / target_area[:, at])
            carry = carry + value
        return carry

    for copy in small[2:]:
        copy.wait()
    target_sum[...] = own_group(0, edge // 2, jnp.zeros((columns, tile), jnp.float32))

    for way, there in ((0, has_high), (1, has_low)):
        @pl.when(there)
        def _(way=way):
            for copy in table_copies(way):
                copy.wait_recv()
            pairs = ((tile_in, tile_n), (block_in, block_n), (live_in, live_n))
            fetch([(a.at[way], b.at[way]) for a, b in pairs])

        @pl.when(jnp.logical_not(there))
        def _(way=way):
            pairs = ((tile_h, tile_n), (block_h, block_n), (live_h, live_n))
            fetch([(a, b.at[way]) for a, b in pairs])

    reaches = (
        (HALO_BLK - own, own - HALO_BLK, own),
        (HALO_BLK + own, 0, HALO_BLK),
    )

    def one_edge(j, carry):
        for way, there in ((0, has_high), (1, has_low)):
            table = (
                lambda k, n, way=way: tile_n[way, k, n],
                lambda k, n, way=way: block_n[way, k, n],
                lambda n, way=way: live_n[way, 0, n],
            )
            first = 0 if way == 0 else targets - edge
            value = slot_dot(source, held, table, first + j, slots, *reaches[way])
            made[way, j] = value.astype(made.dtype)
            carry = carry + value * there.astype(jnp.float32)

        for way, there in ((0, has_high), (1, has_low)):
            @pl.when((j > 0) & there)
            def _(way=way):
                edge_copy(way, j - 1).start()

        return carry

    edge_total = lax.fori_loop(0, edge, one_edge, target_sum[...])
    target_sum[...] = edge_total

    target_sum[...] = own_group(edge // 2, edge // 2, target_sum[...])
    for way, there in ((0, has_high), (1, has_low)):
        @pl.when(there)
        def _(way=way):
            edge_copy(way, edge - 1).start()

    target_total = lax.fori_loop(
        1, targets // edge, lambda g, carry: own_group(g * edge, edge, carry), target_sum[...]
    )
    rows[0:1, :] = row_of(source_sum)
    rows[1:2, :] = row_of(target_total)
    rows[2:3, :] = jnp.broadcast_to(
        jnp.sum(target_area[...], axis=1, keepdims=True), (1, columns)
    )
    rows[3:8, :] = jnp.zeros((5, columns), jnp.float32)

    def row_copy(step):
        return pltpu.make_async_remote_copy(
            src_ref=rows,
            dst_ref=landed.at[step],
            send_sem=row_send.at[step],
            recv_sem=row_recv.at[step],
            device_id=place(step),
            device_id_type=MESH,
        )

    def begin(step, carry):
        row_copy(step).start()
        return carry

    def end(step, carry):
        row_copy(step).wait()
        return carry

    for way, there in ((0, has_low), (1, has_high)):
        @pl.when(there)
        def _(way=way):
            for copy in table_copies(way):
                copy.wait_send()

    lax.fori_loop(1, count, begin, 0)
    landed[0] = rows[...]

    for way, there in ((0, has_low), (1, has_high)):
        @pl.when(there)
        def _(way=way):
            def add(j, carry):
                edge_copy(way, j).wait_recv()
                t = j if way == 0 else targets - edge + j
                at = pl.ds(pl.multiple_of(t * tile, tile), tile)
                share = 1.0 / target_area[:, at]
                raw[t] = raw[t] + came[way, j].astype(jnp.float32) * share
                return carry

            lax.fori_loop(0, edge, add, 0)

    for way, there in ((0, has_high), (1, has_low)):
        @pl.when(there)
        def _(way=way):
            def sent(j, carry):
                edge_copy(way, j).wait_send()
                return carry

            lax.fori_loop(0, edge, sent, 0)

    lax.fori_loop(1, count, end, 0)
    for m in range(mems):
        total = jnp.zeros(rows.shape, jnp.float32)
        for b in range(bands):
            total = total + landed[lax.rem(me - (m * bands + b) + count, count)]
        totals[m] = total
    mine = totals[mem]
    fix = (mine[0:1, :] - mine[1:2, :]) / mine[2:3, :]
    fix_ref[...] = jnp.broadcast_to(fix, (fix_ref.shape[1], fix.shape[1])).T


def main_call(fields, mask, area, target_area, tiles, tile_t, block_t, live):
    bands, mems = lax.axis_size("band"), lax.axis_size("mem")
    rows, snaps, cells = fields.shape
    columns = rows * snaps
    slots, targets = tile_t.shape
    count, tile = tiles.shape[0], tiles.shape[1]
    own = cells // tile
    edge = HALO_BLK // (own // targets)
    dma = pltpu.SemaphoreType.DMA
    peers = bands * mems
    return pl.pallas_call(
        functools.partial(main_kernel, bands, mems, edge),
        in_specs=[HBM] * 8,
        out_specs=(VMEM, VMEM, VMEM),
        out_shape=(
            jax.ShapeDtypeStruct((targets, columns, tile), jnp.float32),
            jax.ShapeDtypeStruct((mems, 8, columns), jnp.float32),
            jax.ShapeDtypeStruct((columns, tile), jnp.float32),
        ),
        scratch_shapes=[
            pltpu.VMEM(mask.shape, mask.dtype),
            pltpu.VMEM(area.shape, area.dtype),
            pltpu.VMEM(target_area.shape, target_area.dtype),
            pltpu.SMEM(tile_t.shape, tile_t.dtype),
            pltpu.SMEM(block_t.shape, block_t.dtype),
            pltpu.SMEM(live.shape, live.dtype),
            pltpu.VMEM(fields.shape, fields.dtype),
            pltpu.VMEM((own, columns, tile), jnp.bfloat16),
            pltpu.VMEM((count + 1, tile, tile), tiles.dtype),
            pltpu.VMEM((2, edge, columns, tile), SEND_TYPE),
            pltpu.VMEM((2, edge, columns, tile), SEND_TYPE),
            pltpu.VMEM((8, columns), jnp.float32),
            pltpu.VMEM((peers, 8, columns), jnp.float32),
            pltpu.VMEM((columns, tile), jnp.float32),
            pltpu.VMEM((2, slots, targets), jnp.int32),
            pltpu.VMEM((2, slots, targets), jnp.int32),
            pltpu.VMEM((2, 1, targets), jnp.int32),
            pltpu.SMEM((2, slots, targets), jnp.int32),
            pltpu.SMEM((2, slots, targets), jnp.int32),
            pltpu.SMEM((2, 1, targets), jnp.int32),
            dma((own // HALO_BLK,)),
            dma((7,)),
            dma((3,)),
            dma((2, 3)),
            dma((2, 3)),
            dma((2, edge)),
            dma((2, edge)),
            dma((peers,)),
            dma((peers,)),
        ],
        compiler_params=pltpu.CompilerParams(
            collective_id=0, has_side_effects=True, vmem_limit_bytes=32 << 20
        ),
    )(*[pltpu.with_memory_space_constraint(a, pltpu.HBM) for a in (fields, mask, area, target_area, tiles, tile_t, block_t, live)])


def finish_kernel(fields, snaps, raw_ref, fix_ref, totals_ref, out_ref, mean_ref, ensemble_ref):
    count, columns, tile = raw_ref.shape
    fix = fix_ref[...]
    for n in range(count):
        value = raw_ref[n] + fix
        out_ref[:, :, n * tile:(n + 1) * tile] = value.reshape(columns // snaps, snaps, tile)

    @pl.when(pl.program_id(0) == 1)
    def _():
        mems, members = totals_ref.shape[0], mean_ref.shape[0]
        spot = lax.broadcasted_iota(jnp.int32, (columns, tile), 0)
        lane = lax.broadcasted_iota(jnp.int32, (columns, tile), 1)
        chosen = lax.rem(spot, snaps) == lane
        summed = jnp.zeros((fields, snaps), jnp.float32)

        def table(m):
            row = totals_ref[m, 0:1, :] / totals_ref[m, 2:3, :]
            column = jnp.broadcast_to(row, (tile, columns)).T
            spread = jnp.where(chosen, column, 0.0).reshape(columns // snaps, snaps, tile)
            return jnp.sum(spread, axis=1)[:, 0:snaps]

        mine = table(lax.axis_index("mem"))
        for n in range(members):
            mean_ref[n] = mine[n * fields:(n + 1) * fields]
        for m in range(mems):
            all_of = table(m)
            for n in range(members):
                summed = summed + all_of[n * fields:(n + 1) * fields]
        ensemble_ref[...] = summed / (mems * members)


def finish(raw, fix, totals, members, fields, snaps):
    targets, columns, tile = raw.shape
    steps = 2
    part = targets // steps
    rows = members * fields
    return pl.pallas_call(
        functools.partial(finish_kernel, fields, snaps),
        grid=(steps,),
        in_specs=[
            pl.BlockSpec((part, columns, tile), lambda i: (i, 0, 0)),
            pl.BlockSpec((columns, tile), lambda i: (0, 0)),
            pl.BlockSpec(totals.shape, lambda i: (0, 0, 0)),
        ],
        out_specs=(
            pl.BlockSpec((rows, snaps, part * tile), lambda i: (0, 0, i)),
            pl.BlockSpec((members, fields, snaps), lambda i: (0, 0, 0)),
            pl.BlockSpec((fields, snaps), lambda i: (0, 0)),
        ),
        out_shape=(
            jax.ShapeDtypeStruct((rows, snaps, targets * tile), jnp.float32),
            jax.ShapeDtypeStruct((members, fields, snaps), jnp.float32),
            jax.ShapeDtypeStruct((fields, snaps), jnp.float32),
        ),
        compiler_params=pltpu.CompilerParams(vmem_limit_bytes=16 << 20),
    )(raw, fix, totals)


def on_device(
    surface_fields, land_mask, source_area, target_area, weight_tiles, tile_of, block_of, live_slots
):
    members, fields, snaps, cells = surface_fields.shape
    targets = tile_of.shape[0]
    target_cells = target_area.shape[0]
    raw, totals, fix = main_call(
        surface_fields.reshape(members * fields, snaps, cells),
        land_mask.reshape(1, cells),
        source_area.reshape(1, cells),
        target_area.reshape(1, target_cells),
        weight_tiles,
        tile_of.T,
        block_of.T,
        live_slots.reshape(1, targets),
    )
    regridded, conserved, ensemble = finish(raw, fix, totals, members, fields, snaps)
    return regridded.reshape(members, fields, snaps, target_cells), conserved, ensemble


def solution(mesh):
    placed = (
        P(("grp", "mem"), "fld", None, "band"),
        P("band"),
        P("band"),
        P("band"),
        P(),
        P("band", None),
        P("band", None),
        P("band"),
    )
    return jax.shard_map(
        on_device,
        mesh=mesh,
        in_specs=placed,
        out_specs=(
            P(("grp", "mem"), "fld", None, "band"),
            P(("grp", "mem"), "fld", None),
            P(("grp", "fld"), None),
        ),
        check_vma=False,
    )
```
